16 devices in a mesh: rep: 4 (over y, z, core), dp: 4 (over x).
Axes of the slice: x: 4, y: 2, z: 1, core: 2. Of those that a mesh axis runs over, the one named last changes fastest.
The devices are a block of a 4x4x8 slice.
Arguments:
- x: bfloat16 [16, 2048, 768], P(('rep', 'dp')), parts along dimension 0
- dy: bfloat16 [16, 2048, 768], P(('rep', 'dp')), parts along dimension 0
- wq: bfloat16 [2, 768, 768], replicated
- wk: bfloat16 [2, 768, 256], replicated
- wv: bfloat16 [2, 768, 256], replicated
- wo: bfloat16 [2, 768, 768], replicated
- w_gate: bfloat16 [2, 768, 2048], replicated
- w_up: bfloat16 [2, 768, 2048], replicated
- w_down: bfloat16 [2, 2048, 768], replicated
- m_wq: float32 [2, 768, 768], P(None, 'dp')
- m_wk: float32 [2, 768, 256], P(None, 'dp')
- m_wv: float32 [2, 768, 256], P(None, 'dp')
- m_wo: float32 [2, 768, 768], P(None, 'dp')
- m_w_gate: float32 [2, 768, 2048], P(None, 'dp')
- m_w_up: float32 [2, 768, 2048], P(None, 'dp')
- m_w_down: float32 [2, 2048, 768], P(None, 'dp')
- v_wq: float32 [2, 768, 768], P(None, 'dp')
- v_wk: float32 [2, 768, 256], P(None, 'dp')
- v_wv: float32 [2, 768, 256], P(None, 'dp')
- v_wo: float32 [2, 768, 768], P(None, 'dp')
- v_w_gate: float32 [2, 768, 2048], P(None, 'dp')
- v_w_up: float32 [2, 768, 2048], P(None, 'dp')
- v_w_down: float32 [2, 2048, 768], P(None, 'dp')
Outputs:
- output 1: bfloat16 [8, 768, 768], P('rep'), parts along dimension 0
- output 2: bfloat16 [8, 768, 256], P('rep'), parts along dimension 0
- output 3: bfloat16 [8, 768, 256], P('rep'), parts along dimension 0
- output 4: bfloat16 [8, 768, 768], P('rep'), parts along dimension 0
- output 5: bfloat16 [8, 768, 2048], P('rep'), parts along dimension 0
- output 6: bfloat16 [8, 768, 2048], P('rep'), parts along dimension 0
- output 7: bfloat16 [8, 2048, 768], P('rep'), parts along dimension 0
- output 8: float32 [8, 768, 768], P('rep', 'dp'), parts along dimension 0
- output 9: float32 [8, 768, 256], P('rep', 'dp'), parts along dimension 0
- output 10: float32 [8, 768, 256], P('rep', 'dp'), parts along dimension 0
- output 11: float32 [8, 768, 768], P('rep', 'dp'), parts along dimension 0
- output 12: float32 [8, 768, 2048], P('rep', 'dp'), parts along dimension 0
- output 13: float32 [8, 768, 2048], P('rep', 'dp'), parts along dimension 0
- output 14: float32 [8, 2048, 768], P('rep', 'dp'), parts along dimension 0
- output 15: float32 [8, 768, 768], P('rep', 'dp'), parts along dimension 0
- output 16: float32 [8, 768, 256], P('rep', 'dp'), parts along dimension 0
- output 17: float32 [8, 768, 256], P('rep', 'dp'), parts along dimension 0
- output 18: float32 [8, 768, 768], P('rep', 'dp'), parts along dimension 0
- output 19: float32 [8, 768, 2048], P('rep', 'dp'), parts along dimension 0
- output 20: float32 [8, 768, 2048], P('rep', 'dp'), parts along dimension 0
- output 21: float32 [8, 2048, 768], P('rep', 'dp'), parts along dimension 0
There are 4 independent parts. The reference program is written for one: setup_inputs(seed, part) draws one part's arguments, and reference() takes and returns one part's arrays. A program takes and returns all parts, laid end to end along the dimension named above; an argument that names none is the same for every part.
All inputs are finite; a program needn't handle non-finite values.
Results may differ from the reference program's by a relative error of at most 0.024.
Values are sent between devices in bfloat16 or wider.
A program may use at most 768 MiB of HBM per device.

```python
import jax
import jax.numpy as jnp
from jax import lax

SEQUENCES = 4
TOKENS = 2048
D = 768
HEADS = 6
KV_HEADS = 2
HEAD = 128
FF = 2048
LAYERS = 2
THETA = 10000
NAMES = ("wq", "wk", "wv", "wo", "w_gate", "w_up", "w_down")
SHAPES = {
    "wq": (LAYERS, D, HEADS * HEAD),
    "wk": (LAYERS, D, KV_HEADS * HEAD),
    "wv": (LAYERS, D, KV_HEADS * HEAD),
    "wo": (LAYERS, HEADS * HEAD, D),
    "w_gate": (LAYERS, D, FF),
    "w_up": (LAYERS, D, FF),
    "w_down": (LAYERS, FF, D),
}


def bump(key, n, height):
    away = (jnp.arange(n, dtype=jnp.int32) - jax.random.randint(key, (), 0, n, jnp.int32)) % n
    return jnp.where(away < n // 8, height, 1.0)


def together(key, own, strength):
    shared = jax.random.normal(key, own.shape[1:], jnp.float32)
    return (own + strength * shared) * lax.rsqrt(1 + strength * strength)


def setup_inputs(seed: int = 0, part: int = 0) -> dict:
    kx, kdy, ka, kb, kz, kf, kh, kl, *keys = jax.random.split(jax.random.key(seed), 8 + 3 * len(NAMES))
    kx, kdy, ka, kb = (jax.random.fold_in(k, part) for k in (kx, kdy, ka, kb))
    kw, km, kv = (keys[i::3] for i in range(3))
    shape = (SEQUENCES, TOKENS, D)
    much_x, much_dy = jax.random.uniform(kz, (2,), jnp.float32, 0.0, 1.0)
    loud = 2.0 ** jax.random.uniform(jax.random.fold_in(kz, 1), (), jnp.float32, -1.0, 2.0)
    layers = 2.0 ** jax.random.uniform(kl, (LAYERS, 1, 1), jnp.float32, -1.0, 1.0)
    times = {"wq": 1.0, "wk": 1.0, "wv": 2.0, "wo": layers, "w_gate": 1.0, "w_up": bump(kh, FF, 4.0), "w_down": layers}
    x = together(ka, jax.random.normal(kx, shape, jnp.float32), much_x) * bump(kf, D, 4.0)
    dy = together(kb, jax.random.normal(kdy, shape, jnp.float32), much_dy)
    drawn = {"x": x.astype(jnp.bfloat16), "dy": (loud * dy * (SEQUENCES * TOKENS) ** -0.5).astype(jnp.bfloat16)}
    for key, name in zip(kw, NAMES, strict=True):
        drawn[name] = (jax.random.normal(key, SHAPES[name], jnp.float32) * SHAPES[name][1] ** -0.5 * times[name]).astype(jnp.bfloat16)
    for key, name in zip(km, NAMES, strict=True):
        drawn[f"m_{name}"] = 0.1 * jax.random.normal(key, SHAPES[name], jnp.float32)
    for key, name in zip(kv, NAMES, strict=True):
        drawn[f"v_{name}"] = jax.random.uniform(key, SHAPES[name], jnp.float32, 0.02, 0.06)
    return drawn


def matmul(a, w):
    return jnp.dot(a, w, preferred_element_type=jnp.float32).astype(jnp.bfloat16)


def normed(h):
    wide = h.astype(jnp.float32)
    scale = lax.rsqrt(jnp.mean(wide**2, -1, keepdims=True) + 1e-6)
    return (wide * scale).astype(jnp.bfloat16)


def turned(t, theta):
    half = t.shape[-1] // 2
    angle = jnp.arange(t.shape[0], dtype=jnp.float32)[:, None] * theta ** (-jnp.arange(half, dtype=jnp.float32) / half)
    cos, sin = jnp.cos(angle)[:, None], jnp.sin(angle)[:, None]
    a, b = t[..., :half].astype(jnp.float32), t[..., half:].astype(jnp.float32)
    return jnp.concatenate([a * cos - b * sin, b * cos + a * sin], -1).astype(jnp.bfloat16)


def seen_by(q, k, v):
    tokens, kv = q.shape[0], k.shape[1]
    q = q.reshape(tokens, kv, -1, q.shape[-1])
    scores = jnp.einsum("tgsd,ugd->gstu", q.astype(jnp.float32), k.astype(jnp.float32)) * q.shape[-1] ** -0.5
    place = jnp.arange(tokens)
    weights = jax.nn.softmax(jnp.where(place[:, None] >= place, scores, -jnp.inf), -1).astype(jnp.bfloat16)
    return jnp.einsum("gstu,ugd->tgsd", weights.astype(jnp.float32), v.astype(jnp.float32)).astype(jnp.bfloat16).reshape(tokens, -1)


def layer(h, w):
    a = normed(h)
    q, k = (turned(matmul(a, w[name]).reshape(h.shape[0], -1, HEAD), THETA) for name in ("wq", "wk"))
    h = h + matmul(seen_by(q, k, matmul(a, w["wv"]).reshape(h.shape[0], -1, HEAD)), w["wo"])
    b = normed(h)
    gate = jnp.dot(b, w["w_gate"], preferred_element_type=jnp.float32)
    up = jnp.dot(b, w["w_up"], preferred_element_type=jnp.float32)
    return h + matmul((jax.nn.silu(gate) * up).astype(jnp.bfloat16), w["w_down"])


def adamw(w, m, v, g):
    m = 0.9 * m + 0.1 * g
    v = 0.95 * v + 0.05 * g * g
    step = m * lax.rsqrt(v + 1e-8) + 0.1 * w
    return (w - 0.02 * step).astype(jnp.bfloat16), m, v


def clipped(gradients, sum_of_squares, count):
    factor = jnp.minimum(1.0, 0.5 * lax.rsqrt(sum_of_squares / count + 1e-30))
    return [g * factor for g in gradients]


def stack(weights, h):
    return lax.scan(lambda h, w: (layer(h, w), None), h, weights)[0]


def reference(x, dy, wq, wk, wv, wo, w_gate, w_up, w_down, m_wq, m_wk, m_wv, m_wo, m_w_gate, m_w_up, m_w_down, v_wq, v_wk, v_wv, v_wo, v_w_gate, v_w_up, v_w_down):
    weights = dict(zip(NAMES, (wq, wk, wv, wo, w_gate, w_up, w_down), strict=True))

    def take(so_far, sequence):
        h, by_y = sequence
        _, back = jax.vjp(stack, weights, h)
        by_weights, by_h = back(by_y)
        return jax.tree.map(lambda total, term: total + term.astype(jnp.float32), so_far, by_weights), by_h

    none_yet = {name: jnp.zeros(w.shape, jnp.float32) for name, w in weights.items()}
    by_weights, by_x = lax.scan(take, none_yet, (x, dy))
    gradients = [by_weights[name].astype(jnp.bfloat16).astype(jnp.float32) for name in NAMES]
    gradients = clipped(gradients, sum(jnp.sum(g * g) for g in gradients), sum(g.size for g in gradients))
    first = (m_wq, m_wk, m_wv, m_wo, m_w_gate, m_w_up, m_w_down)
    second = (v_wq, v_wk, v_wv, v_wo, v_w_gate, v_w_up, v_w_down)
    new = [adamw(weights[name].astype(jnp.float32), m, v, g) for name, m, v, g in zip(NAMES, first, second, gradients, strict=True)]
    return tuple(one[which] for which in range(3) for one in new)
```

```python
import functools

import jax
import jax.numpy as jnp
from jax import lax
from jax.experimental import pallas as pl
from jax.experimental.pallas import tpu as pltpu
from jax.sharding import PartitionSpec as P

HEAD = 128
THETA = 10000
EPS = 1e-6
LOG2E = 1.4426950408889634
LOW = -1e30
VMEM = 60 * 2**20
NAMES = ("wq", "wk", "wv", "wo", "w_gate", "w_up", "w_down")
F32, BF16 = jnp.float32, jnp.bfloat16


def dot(a, b, ca=1, cb=0):
    return lax.dot_general(a, b, (((ca,), (cb,)), ((), ())), preferred_element_type=F32)


def fit(size, want):
    while size % want:
        want //= 2
    return want


def call(kernel, grid, ins, outs, out_shape, scratch=(), flops=0, exps=0, order=None):
    arrays = [a for a, _ in ins]
    moved = sum(a.size * a.dtype.itemsize for a in arrays) + sum(o.size * o.dtype.itemsize for o in out_shape)
    return pl.pallas_call(
        kernel, grid=grid, in_specs=[s for _, s in ins], out_specs=outs, out_shape=out_shape, scratch_shapes=list(scratch),
        compiler_params=pltpu.CompilerParams(dimension_semantics=("arbitrary",) * len(grid), vmem_limit_bytes=VMEM),
        cost_estimate=pl.CostEstimate(flops=flops, transcendentals=exps, bytes_accessed=moved),
    )(*arrays)


def rows(bt, width):
    return pl.BlockSpec((bt, width), lambda i: (i, 0))


def columns(height, bt):
    return pl.BlockSpec((height, bt), lambda i: (0, i))


def whole(w, number):
    return w, pl.BlockSpec((None, *w.shape[1:]), lambda *_: (number, 0, 0), pipeline_mode=pl.Buffered(1))


def shape(*s, dtype=BF16):
    return jax.ShapeDtypeStruct(s, dtype)


def normed(h):
    scale = lax.rsqrt(jnp.mean(h * h, -1, keepdims=True) + EPS)
    return (h * scale).astype(BF16), scale


def norm_back(h, by_b):
    scale = lax.rsqrt(jnp.mean(h * h, -1, keepdims=True) + EPS)
    along = jnp.mean(h * by_b, -1, keepdims=True)
    return (by_b - h * (along * scale * scale)) * scale


def turn(t, cos, sin):
    t = t.astype(F32)
    return (t * cos + pltpu.roll(t, HEAD // 2, 1) * sin).astype(BF16)


def tables(tokens):
    half = HEAD // 2
    angle = jnp.arange(tokens, dtype=F32)[:, None] * THETA ** (-jnp.arange(half, dtype=F32) / half)
    cos, sin = jnp.cos(angle), jnp.sin(angle)
    return jnp.concatenate([cos, cos], 1), jnp.concatenate([-sin, sin], 1)


def _project(h_ref, wq_ref, wk_ref, wv_ref, cos_ref, sin_ref, q_ref, k_ref, v_ref, a_ref):
    a, _ = normed(h_ref[...].astype(F32))
    a_ref[...] = a.T
    cos, sin = cos_ref[...], sin_ref[...]
    for w_ref, o_ref in ((wq_ref, q_ref), (wk_ref, k_ref)):
        t = dot(a, w_ref[...]).astype(BF16)
        for at in range(0, t.shape[1], HEAD):
            o_ref[:, at : at + HEAD] = turn(t[:, at : at + HEAD], cos, sin)
    v_ref[...] = dot(a, wv_ref[...]).astype(BF16)


def project(h, weights, number, cos, sin, bt=512):
    t, d = h.shape
    bt = fit(t, bt)
    wq, wk, wv = weights[:3]
    nq, nk = wq.shape[2], wk.shape[2]
    return call(_project, (t // bt,),
                [(h, rows(bt, d)), whole(wq, number), whole(wk, number), whole(wv, number), (cos, rows(bt, HEAD)), (sin, rows(bt, HEAD))],
                [rows(bt, nq), rows(bt, nk), rows(bt, nk), columns(d, bt)], [shape(t, nq), shape(t, nk), shape(t, nk), shape(d, t)],
                flops=2 * t * d * (nq + 2 * nk))


def _spans(iq, b, block):
    lax.fori_loop(0, iq, lambda j, _: block(pl.multiple_of(j * b, b), b, 0, False), None)
    block(pl.multiple_of(iq * b, b), b // 2, 0, True)
    block(pl.multiple_of(iq * b + b // 2, b // 2), b // 2, b // 2, True)


def _attend(q_ref, k_ref, v_ref, o_ref, turned_ref, lse_ref, top_s, mix_s, *, kv, g, b):
    e = HEAD**-0.5 * LOG2E
    heads = [(i, i * g + n) for i in range(kv) for n in range(g)]
    top_s[...] = jnp.full(top_s.shape, LOW, F32)
    mix_s[...] = jnp.zeros(mix_s.shape, F32)

    def block(at, size, first, masked):
        width = b - first
        here = pl.ds(at, size)
        scores = [dot(k_ref[here, i * HEAD : (i + 1) * HEAD], q_ref[first:, n * HEAD : (n + 1) * HEAD], 1, 1) for i, n in heads]
        if masked:
            ok = lax.broadcasted_iota(jnp.int32, (size, width), 1) >= lax.broadcasted_iota(jnp.int32, (size, width), 0)
        parts, keeps = [], []
        for (_, n), s in zip(heads, scores):
            if masked:
                s = jnp.where(ok, s, 2 * LOW)
            old = top_s[n : n + 1, first:]
            top = jnp.maximum(old, s.max(axis=0, keepdims=True))
            top_s[n : n + 1, first:] = top
            parts.append(jnp.exp2((s - top) * e).astype(BF16))
            keeps.append(jnp.exp2((old - top) * e))
        ones = jnp.ones((8, size), BF16)
        for (i, n), p, keep in zip(heads, parts, keeps):
            values = jnp.concatenate([v_ref[here, i * HEAD : (i + 1) * HEAD].T, ones], axis=0)
            mix_s[n, :, first:] = mix_s[n, :, first:] * keep + dot(values, p)

    _spans(pl.program_id(0), b, block)
    for i, n in heads:
        total = mix_s[n, HEAD : HEAD + 1, :]
        out = mix_s[n, :HEAD, :] * (1 / total)
        turned_ref[n * HEAD : (n + 1) * HEAD, :] = out.astype(BF16)
        o_ref[:, n * HEAD : (n + 1) * HEAD] = out.T.astype(BF16)
        lse_ref[n : n + 1, :] = top_s[n : n + 1, :] * e + jnp.log2(total)


def attend(q, k, v, b=512):
    t, width = q.shape
    b = fit(t, b)
    kv, heads = k.shape[1] // HEAD, width // HEAD
    keys = pl.BlockSpec(k.shape, lambda i: (0, 0), pipeline_mode=pl.Buffered(1))
    return call(functools.partial(_attend, kv=kv, g=heads // kv, b=b), (t // b,), [(q, rows(b, width)), (k, keys), (v, keys)],
                [rows(b, width), columns(width, b), columns(heads, b)], [shape(t, width), shape(width, t), shape(heads, t, dtype=F32)],
                [pltpu.VMEM((heads, b), F32), pltpu.VMEM((heads, HEAD + 8, b), F32)],
                flops=2 * t * t * width, exps=heads * t * t // 2)


def _feed(o_ref, h_ref, wo_ref, wg_ref, wu_ref, wd_ref, h2_ref, b_ref, gate_ref, up_ref, act_ref, h3_ref, act_s):
    h2 = (h_ref[...].astype(F32) + dot(o_ref[...], wo_ref[...]).astype(BF16).astype(F32)).astype(BF16)
    h2_ref[...] = h2
    b, _ = normed(h2.astype(F32))
    b_ref[...] = b.T
    for at in range(0, wg_ref.shape[1], 512):
        c = slice(at, at + 512)
        gate, up = dot(b, wg_ref[:, c]), dot(b, wu_ref[:, c])
        gate_ref[:, c] = gate
        up_ref[:, c] = up
        act = (gate * jax.nn.sigmoid(gate) * up).astype(BF16)
        act_ref[c, :] = act.T
        if h3_ref is not None:
            act_s[:, c] = act
    if h3_ref is not None:
        h3_ref[...] = (h2.astype(F32) + dot(act_s[...], wd_ref[...]).astype(BF16).astype(F32)).astype(BF16)


def feed(o, h, weights, number, last, bt=512):
    t, d = h.shape
    bt = fit(t, bt)
    wo, wg, wu, wd = weights[3:]
    f = wg.shape[2]
    ins = [(o, rows(bt, o.shape[1])), (h, rows(bt, d)), *(whole(w, number) for w in ((wo, wg, wu) if last else (wo, wg, wu, wd)))]
    specs = [rows(bt, d), columns(d, bt), rows(bt, f), rows(bt, f), columns(f, bt)] + ([] if last else [rows(bt, d)])
    shapes = [shape(t, d), shape(d, t), shape(t, f, dtype=F32), shape(t, f, dtype=F32), shape(f, t)] + ([] if last else [shape(t, d)])

    def kernel(*refs):
        _feed(*refs[:5], None, *refs[5:], None, None) if last else _feed(*refs)

    return call(kernel, (t // bt,), ins, specs, shapes, [] if last else [pltpu.VMEM((bt, f), BF16)],
                flops=2 * t * d * (o.shape[1] + (2 if last else 3) * f), exps=t * f)


def _feed_back(dh_ref, h2_ref, gate_ref, up_ref, wo_ref, wg_ref, wu_ref, wd_ref, dgu_ref, dh2_ref, do_ref):
    dh, f = dh_ref[...], wg_ref.shape[1]
    for at in range(0, f, 512):
        c = slice(at, at + 512)
        dact = dot(dh, wd_ref[c, :], 1, 1).astype(BF16).astype(F32)
        gate, up = gate_ref[:, c], up_ref[:, c]
        sig = jax.nn.sigmoid(gate)
        s = gate * sig
        dgu_ref[:, f + at : f + at + 512] = (dact * s).astype(BF16)
        dgu_ref[:, c] = (dact * up * (sig + s * (1 - sig))).astype(BF16)
    db = dot(dgu_ref[:, :f], wg_ref[...], 1, 1) + dot(dgu_ref[:, f:], wu_ref[...], 1, 1)
    by_h = norm_back(h2_ref[...].astype(F32), db.astype(BF16).astype(F32)).astype(BF16)
    dh2 = (dh.astype(F32) + by_h.astype(F32)).astype(BF16)
    dh2_ref[...] = dh2
    do_ref[...] = dot(dh2, wo_ref[...], 1, 1).astype(BF16)


def feed_back(dh, h2, gate, up, weights, number, bt=512):
    t, d = dh.shape
    bt = fit(t, bt)
    f, n = gate.shape[1], weights[3].shape[1]
    return call(_feed_back, (t // bt,),
                [(dh, rows(bt, d)), (h2, rows(bt, d)), (gate, rows(bt, f)), (up, rows(bt, f)), *(whole(w, number) for w in weights[3:])],
                [rows(bt, 2 * f), rows(bt, d), rows(bt, n)], [shape(t, 2 * f), shape(t, d), shape(t, n)],
                flops=2 * t * d * (3 * f + n), exps=t * f)


def _attend_back(q_ref, k_ref, v_ref, o_ref, do_ref, lse_ref, cos_ref, sin_ref, dq_ref, dk_ref, dv_ref, dq_s, dk_s, dv_s, *, kv, g, b):
    iq = pl.program_id(0)
    scale = HEAD**-0.5
    e = scale * LOG2E

    @pl.when(iq == 0)
    def _():
        dk_s[...] = jnp.zeros_like(dk_s)
        dv_s[...] = jnp.zeros_like(dv_s)

    dq_s[...] = jnp.zeros_like(dq_s)
    column = lambda n: slice(n * HEAD, (n + 1) * HEAD)
    deltas = [(do_ref[:, column(n)].astype(F32) * o_ref[:, column(n)].astype(F32)).T.sum(0, keepdims=True) for n in range(kv * g)]

    def block(at, size, first, masked):
        width = b - first
        here = pl.ds(at, size)
        if masked:
            ok = lax.broadcasted_iota(jnp.int32, (size, width), 1) >= lax.broadcasted_iota(jnp.int32, (size, width), 0)
        for i in range(kv):
            key, value = k_ref[here, column(i)], v_ref[here, column(i)]
            group = range(i * g, (i + 1) * g)
            qs = [q_ref[first:, column(n)] for n in group]
            dos = [do_ref[first:, column(n)] for n in group]
            scores = [dot(key, x, 1, 1) for x in qs]
            dps = [dot(value, x, 1, 1) for x in dos]
            ps, dss = [], []
            for n, s, dp in zip(group, scores, dps):
                p = jnp.exp2(s * e - lse_ref[n : n + 1, first:])
                if masked:
                    p = jnp.where(ok, p, 0.0)
                ps.append(p.astype(BF16))
                dss.append((p * (dp - deltas[n][:, first:])).astype(BF16))
            dv_s[i, here, :] += dot(jnp.concatenate(ps, 1), jnp.concatenate(dos, 0))
            dk_s[i, here, :] += dot(jnp.concatenate(dss, 1), jnp.concatenate(qs, 0))
            back = key.T
            for n, ds in zip(group, dss):
                dq_s[n, :, first:] += dot(back, ds)

    _spans(iq, b, block)
    mine = pl.ds(pl.multiple_of(iq * b, b), b)
    cos, sin = cos_ref[mine, :], -sin_ref[mine, :]
    for n in range(kv * g):
        dq_ref[:, column(n)] = turn((dq_s[n] * scale).T.astype(BF16), cos, sin)

    @pl.when(iq == pl.num_programs(0) - 1)
    def _():
        for i in range(kv):
            dk_ref[:, column(i)] = turn((dk_s[i] * scale).astype(BF16), cos_ref[...], -sin_ref[...])
            dv_ref[:, column(i)] = dv_s[i].astype(BF16)


def attend_back(q, k, v, o, do, lse, cos, sin, b=512):
    t, width = q.shape
    b = fit(t, b)
    kv, heads = k.shape[1] // HEAD, width // HEAD
    fixed = lambda a: pl.BlockSpec(a.shape, lambda i: (0, 0), pipeline_mode=pl.Buffered(1))
    keys = pl.BlockSpec(k.shape, lambda i: (0, 0))
    return call(functools.partial(_attend_back, kv=kv, g=heads // kv, b=b), (t // b,),
                [(q, rows(b, width)), (k, fixed(k)), (v, fixed(v)), (o, rows(b, width)), (do, rows(b, width)),
                 (lse, pl.BlockSpec((heads, b), lambda i: (0, i))), (cos, fixed(cos)), (sin, fixed(sin))],
                [rows(b, width), keys, keys], [shape(t, width), shape(*k.shape), shape(*v.shape)],
                [pltpu.VMEM((heads, HEAD, b), F32), pltpu.VMEM((kv, t, HEAD), F32), pltpu.VMEM((kv, t, HEAD), F32)],
                flops=5 * t * t * width, exps=heads * t * t // 2)


def _project_back(dq_ref, dk_ref, dv_ref, h_ref, dh2_ref, wq_ref, wk_ref, wv_ref, dh_ref):
    da = dot(dq_ref[...], wq_ref[...], 1, 1) + dot(dk_ref[...], wk_ref[...], 1, 1) + dot(dv_ref[...], wv_ref[...], 1, 1)
    by_h = norm_back(h_ref[...].astype(F32), da.astype(BF16).astype(F32)).astype(BF16)
    dh_ref[...] = (dh2_ref[...].astype(F32) + by_h.astype(F32)).astype(BF16)


def project_back(dq, dk, dv, h, dh2, weights, number, bt=512):
    t, d = h.shape
    bt = fit(t, bt)
    return call(_project_back, (t // bt,),
                [(dq, rows(bt, dq.shape[1])), (dk, rows(bt, dk.shape[1])), (dv, rows(bt, dv.shape[1])), (h, rows(bt, d)), (dh2, rows(bt, d)),
                 *(whole(w, number) for w in weights[:3])],
                [rows(bt, d)], [shape(t, d)], flops=2 * t * d * (dq.shape[1] + 2 * dk.shape[1]))[0]


def _product(a_ref, b_ref, o_ref):
    o_ref[...] = dot(a_ref[...], b_ref[...]).astype(BF16)


def by_columns(a, b, bn=512):
    (m, t), n = a.shape, b.shape[1]
    bn = fit(n, bn)
    return call(_product, (n // bn,), [(a, pl.BlockSpec((m, t), lambda i: (0, 0), pipeline_mode=pl.Buffered(1))), (b, columns(t, bn))],
                [columns(m, bn)], [shape(m, n)], flops=2 * m * t * n)[0]


def by_rows(a, b, bm=512):
    (m, t), n = a.shape, b.shape[1]
    bm = fit(m, bm)
    return call(_product, (m // bm,), [(a, rows(bm, t)), (b, pl.BlockSpec((t, n), lambda i: (0, 0), pipeline_mode=pl.Buffered(1)))],
                [rows(bm, n)], [shape(m, n)], flops=2 * m * t * n)[0]


def by_attention(a, o, dq, dh2, dk, dv, bn=256):
    m, t = a.shape
    right = (dq, dh2, dk, dv)
    ends, at = [], 0
    for one in right:
        at += one.shape[1] // bn
        ends.append(at)
    starts = [0] + ends[:-1]

    def kernel(a_ref, o_ref, *rest):
        for which in range(4):
            @pl.when((pl.program_id(0) >= starts[which]) & (pl.program_id(0) < ends[which]))
            def _():
                _product(o_ref if which == 1 else a_ref, rest[which], rest[4])

    kept = pl.BlockSpec((m, t), lambda i: (0, 0), pipeline_mode=pl.Buffered(1))
    blocks = [pl.BlockSpec((t, bn), lambda i, lo=lo, hi=hi: (0, jnp.clip(i - lo, 0, hi - lo - 1))) for lo, hi in zip(starts, ends)]
    return call(kernel, (at,), [(a, kept), (o, kept), *zip(right, blocks)], [columns(m, bn)], [shape(m, at * bn)], flops=2 * m * t * at * bn)[0]


def _update(me_ref, factor_ref, *refs, count, layers):
    layer = pl.program_id(0)
    gs, refs = refs[:layers], refs[layers:]
    ins, outs = refs[: 3 * count], refs[3 * count :]
    g_s = outs[-1]
    for number in range(layers):
        @pl.when(layer == number)
        def _():
            g_s[...] = gs[number][...].astype(F32) * factor_ref[0, 0]
    at = 0
    for i in range(count):
        w, m, v = (ref[...] for ref in ins[3 * i : 3 * i + 3])
        here = slice(at, at + m.shape[1])
        at += m.shape[1]
        g, w = g_s[:, here], w.astype(F32)
        m = 0.9 * m + 0.1 * g
        v = 0.95 * v + 0.05 * g * g
        outs[1 + 2 * i][...] = m
        outs[2 + 2 * i][...] = v
        outs[0][:, here] = (w - 0.02 * (m * lax.rsqrt(v + 1e-8) + 0.1 * w)).astype(BF16)


def update(me, factor, gradients, members, column):
    layers, r, _ = members[0][1].shape
    total = sum(m.shape[2] for _, m, _ in members)
    bt = r // 4
    steps = r // bt
    block = lambda n: pl.BlockSpec((None, bt, n), lambda l, i, me: (l, i, 0))
    ins, specs = [], []
    for number, g in enumerate(gradients):
        ins.append(g)
        specs.append(pl.BlockSpec((bt, total), lambda l, i, me, number=number: (jnp.where(l == number, i, jnp.where(l < number, 0, steps - 1)), column // total)))
    for w, m, v in members:
        n = m.shape[2]
        ins += [w, m, v]
        specs += [pl.BlockSpec((None, bt, n), lambda l, i, me: (l, me[0] * steps + i, 0)), block(n), block(n)]
    outs = [shape(layers, r, total)] + [shape(*m.shape, dtype=F32) for _, m, _ in members for _ in range(2)]
    return pl.pallas_call(
        functools.partial(_update, count=len(members), layers=layers),
        grid_spec=pltpu.PrefetchScalarGridSpec(
            num_scalar_prefetch=1, grid=(layers, steps),
            in_specs=[pl.BlockSpec(memory_space=pltpu.SMEM), *specs],
            out_specs=[block(total)] + [block(m.shape[2]) for _, m, _ in members for _ in range(2)],
            scratch_shapes=[pltpu.VMEM((bt, total), F32)]),
        out_shape=outs,
        compiler_params=pltpu.CompilerParams(dimension_semantics=("arbitrary", "arbitrary"), vmem_limit_bytes=VMEM),
        cost_estimate=pl.CostEstimate(flops=12 * layers * r * total, transcendentals=layers * r * total, bytes_accessed=22 * layers * r * total),
    )(me, factor, *ins)


def _place(own_ref, left_ref, right_ref, top_ref, bottom_ref, *outs):
    me, n, r = lax.axis_index("dp"), lax.axis_size("dp"), own_ref.shape[0]
    at = 0
    for out in outs:
        here = slice(at, at + out.shape[1])
        at += out.shape[1]
        for source, ref, low in ((0, own_ref, 0), (n - 1, left_ref, 0), (1, right_ref, 0), (2, top_ref, 0), (2, bottom_ref, r // 2)):
            first = pl.multiple_of(lax.rem(me + source, n) * r + low, r // 2)
            out[pl.ds(first, ref.shape[0]), :] = ref[:, here]


def place(pieces, widths, n):
    layers, r, total = pieces[0].shape
    block = lambda rows, columns: pl.BlockSpec((None, rows, columns), lambda l: (l, 0, 0))
    return call(_place, (layers,), [(p, block(p.shape[1], total)) for p in pieces], [block(n * r, c) for c in widths],
                [shape(layers, n * r, c) for c in widths], flops=layers * n * r * total)


def gather(own, n):
    right, left = [(i, (i + 1) % n) for i in range(n)], [(i, (i - 1) % n) for i in range(n)]
    half = own.shape[1] // 2
    a, b = lax.ppermute(own, "dp", right), lax.ppermute(own, "dp", left)
    return own, a, b, lax.ppermute(a[:, :half], "dp", right), lax.ppermute(b[:, half:], "dp", left)


def solution(mesh):
    def scattered(w):
        return lax.psum_scatter(w, "dp", scatter_dimension=0, tiled=True)

    def step(x, dy, *arrays):
        weights, m, v = (arrays[i : i + 7] for i in (0, 7, 14))
        layers = weights[0].shape[0]
        h, kept = x[0], []
        cos, sin = tables(h.shape[0])
        for number in range(layers):
            q, k, value, a = project(h, weights, number, cos, sin)
            o, turned, lse = attend(q, k, value)
            h2, b, gate, up, act, *out = feed(o, h, weights, number, number == layers - 1)
            kept.append((h, q, k, value, a, o, turned, lse, h2, b, gate, up, act))
            h = out[0] if out else None
        dh, downs, gus, qkvos = dy[0], [None] * layers, [None] * layers, [None] * layers
        together = lax.optimization_barrier
        for number in reversed(range(layers)):
            h, q, k, value, a, o, turned, lse, h2, b, gate, up, act = kept[number]
            before = number + 1 if number + 1 < layers else None
            dh, w_down = together((dh, by_rows(act, dh)))
            downs[number] = scattered(w_down)
            dgu, dh2, do = feed_back(dh, h2, gate, up, weights, number)
            if before is None:
                dgu, downs[number] = together((dgu, downs[number]))
            else:
                dgu, qkvos[before] = together((dgu, qkvos[before]))
            do, w_gu = together((do, by_columns(b, dgu)))
            gus[number] = scattered(w_gu)
            dq, dk, dv = attend_back(q, k, value, o, do, lse, cos, sin)
            if before is not None:
                dq, downs[number] = together((dq, downs[number]))
            w_qkvo = by_attention(a, turned, dq, dh2, dk, dv)
            if number:
                dq, w_qkvo = together((dq, w_qkvo))
                dh = project_back(dq, dk, dv, h, dh2, weights, number)
                dh, gus[number] = together((dh, gus[number]))
            qkvos[number] = scattered(w_qkvo)
        n = lax.axis_size("dp")
        parts = downs + gus + qkvos
        squares = lax.psum(sum(jnp.sum(g.astype(F32) ** 2) for g in parts), "dp")
        factor = jnp.minimum(1.0, 0.5 * lax.rsqrt(squares / (n * sum(g.size for g in parts)) + 1e-30)).reshape(1, 1)
        me = lax.axis_index("dp").astype(jnp.int32).reshape(1)
        new = [None] * 21
        f = weights[4].shape[2]
        token = factor
        for gradients, column, which in ((qkvos, 0, (0, 3, 1, 2)), (downs, 0, (6,)), (gus, 0, (4,)), (gus, f, (5,))):
            own, *moments = update(me, token, gradients, [(weights[i], m[i], v[i]) for i in which], column)
            own, token = together((own, token))
            for at, i in enumerate(which):
                new[7 + i], new[14 + i] = moments[2 * at], moments[2 * at + 1]
            for i, one in zip(which, place(gather(own, n), [weights[i].shape[2] for i in which], n)):
                new[i] = one
        return tuple(new)

    states, all_of, cut = P(("rep", "dp"), None, None), P(None, None, None), P(None, "dp", None)
    return jax.shard_map(
        step,
        mesh=mesh,
        in_specs=(states, states) + (all_of,) * 7 + (cut,) * 14,
        out_specs=(P("rep", None, None),) * 7 + (P("rep", "dp", None),) * 14,
        check_vma=False,
    )
```

```python
import functools

import jax
import jax.numpy as jnp
from jax import lax
from jax.experimental import pallas as pl
from jax.experimental.pallas import tpu as pltpu
from jax.sharding import PartitionSpec as P


HEAD = 128
THETA = 10000
EPS = 1e-6
LOG2E = 1.4426950408889634
LOW = -1e30
VMEM = 60 * 2**20
F32, BF16 = jnp.float32, jnp.bfloat16


def dot(a, b, ca=1, cb=0):
    return lax.dot_general(a, b, (((ca,), (cb,)), ((), ())), preferred_element_type=F32)


def fit(size, want):
    while size % want:
        want //= 2
    return want


def call(kernel, grid, ins, outs, out_shape, scratch=(), flops=0, exps=0, number=0):
    arrays = [a for a, _ in ins]
    moved = sum(a.size * a.dtype.itemsize for a in arrays) + sum(o.size * o.dtype.itemsize for o in out_shape)
    return pl.pallas_call(
        lambda _, *refs: kernel(*refs),
        grid_spec=pltpu.PrefetchScalarGridSpec(num_scalar_prefetch=1, grid=grid, in_specs=[s for _, s in ins], out_specs=outs, scratch_shapes=list(scratch)),
        out_shape=out_shape,
        compiler_params=pltpu.CompilerParams(dimension_semantics=("arbitrary",) * len(grid), vmem_limit_bytes=VMEM),
        cost_estimate=pl.CostEstimate(flops=flops, transcendentals=exps, bytes_accessed=moved),
    )(jnp.full((1,), number, jnp.int32), *arrays)


def rows(bt, width):
    return pl.BlockSpec((bt, width), lambda i, _: (i, 0))


def columns(height, bt):
    return pl.BlockSpec((height, bt), lambda i, _: (0, i))


def whole(w):
    return w, pl.BlockSpec((None, *w.shape[1:]), lambda i, number: (number[0], 0, 0), pipeline_mode=pl.Buffered(1))


def kept(a):
    return pl.BlockSpec(a.shape, lambda i, _: (0, 0), pipeline_mode=pl.Buffered(1))


def shape(*s, dtype=BF16):
    return jax.ShapeDtypeStruct(s, dtype)


def sigmoid(x):
    return 0.5 * jnp.tanh(0.5 * x) + 0.5


def normed(h):
    scale = lax.rsqrt(jnp.mean(h * h, -1, keepdims=True) + EPS)
    return (h * scale).astype(BF16), scale


def norm_back(h, by_b):
    scale = lax.rsqrt(jnp.mean(h * h, -1, keepdims=True) + EPS)
    along = jnp.mean(h * by_b, -1, keepdims=True)
    return (by_b - h * (along * scale * scale)) * scale


def turn(t, cos, sin):
    t = t.astype(F32)
    return (t * cos + pltpu.roll(t, HEAD // 2, 1) * sin).astype(BF16)


def tables(tokens):
    half, step = HEAD // 2, 64
    rate = THETA ** (-jnp.arange(half, dtype=F32) / half)
    rate, sign = jnp.concatenate([rate, rate]), jnp.concatenate([-jnp.ones(half, F32), jnp.ones(half, F32)])
    coarse = (jnp.arange(tokens // step, dtype=F32) * step)[:, None] * rate
    fine = jnp.arange(step, dtype=F32)[:, None] * rate
    cc, sc, cf, sf = lax.optimization_barrier((jnp.cos(coarse), jnp.sin(coarse) * sign, jnp.cos(fine), jnp.sin(fine)))
    cos = cc[:, None] * cf - sc[:, None] * sign * sf
    sin = sc[:, None] * cf + cc[:, None] * sign * sf
    return cos.reshape(tokens, HEAD), sin.reshape(tokens, HEAD)


def _project(h_ref, wq_ref, wk_ref, wv_ref, cos_ref, sin_ref, q_ref, k_ref, v_ref, a_ref):
    a, _ = normed(h_ref[...].astype(F32))
    a_ref[...] = a.T
    cos, sin = cos_ref[...], sin_ref[...]
    for w_ref, o_ref in ((wq_ref, q_ref), (wk_ref, k_ref)):
        t = dot(a, w_ref[...]).astype(BF16)
        for at in range(0, t.shape[1], HEAD):
            o_ref[:, at : at + HEAD] = turn(t[:, at : at + HEAD], cos, sin)
    v_ref[...] = dot(a, wv_ref[...]).astype(BF16)


def project(h, weights, number, cos, sin, bt=512):
    t, d = h.shape
    bt = fit(t, bt)
    wq, wk, wv = weights[:3]
    nq, nk = wq.shape[2], wk.shape[2]
    return call(_project, (t // bt,),
                [(h, rows(bt, d)), whole(wq), whole(wk), whole(wv), (cos, rows(bt, HEAD)), (sin, rows(bt, HEAD))],
                [rows(bt, nq), rows(bt, nk), rows(bt, nk), columns(d, bt)], [shape(t, nq), shape(t, nk), shape(t, nk), shape(d, t)],
                flops=2 * t * d * (nq + 2 * nk), number=number)


def _spans(iq, b, block):
    lax.fori_loop(0, iq, lambda j, _: block(pl.multiple_of(j * b, b), b, 0, False), None)
    block(pl.multiple_of(iq * b, b), b // 2, 0, True)
    block(pl.multiple_of(iq * b + b // 2, b // 2), b // 2, b // 2, True)


def _attend(q_ref, k_ref, v_ref, o_ref, turned_ref, lse_ref, top_s, mix_s, *, kv, g, b):
    e = HEAD**-0.5 * LOG2E
    heads = [(i, i * g + n) for i in range(kv) for n in range(g)]
    top_s[...] = jnp.full(top_s.shape, LOW, F32)
    mix_s[...] = jnp.zeros(mix_s.shape, F32)

    def block(at, size, first, masked):
        width = b - first
        here = pl.ds(at, size)
        scores = [dot(k_ref[here, i * HEAD : (i + 1) * HEAD], q_ref[first:, n * HEAD : (n + 1) * HEAD], 1, 1) for i, n in heads]
        if masked:
            ok = lax.broadcasted_iota(jnp.int32, (size, width), 1) >= lax.broadcasted_iota(jnp.int32, (size, width), 0)
        parts, keeps = [], []
        for (_, n), s in zip(heads, scores):
            if masked:
                s = jnp.where(ok, s, 2 * LOW)
            old = top_s[n : n + 1, first:]
            top = jnp.maximum(old, s.max(axis=0, keepdims=True))
            top_s[n : n + 1, first:] = top
            parts.append(jnp.exp2((s - top) * e).astype(BF16))
            keeps.append(jnp.exp2((old - top) * e))
        ones = jnp.ones((8, size), BF16)
        values = [jnp.concatenate([v_ref[here, i * HEAD : (i + 1) * HEAD].T, ones], axis=0) for i in range(kv)]
        for (i, n), p, keep in zip(heads, parts, keeps):
            mix_s[n, :, first:] = mix_s[n, :, first:] * keep + dot(values[i], p)

    _spans(pl.program_id(0), b, block)
    for i, n in heads:
        total = mix_s[n, HEAD : HEAD + 1, :]
        out = mix_s[n, :HEAD, :] * (1 / total)
        turned_ref[n * HEAD : (n + 1) * HEAD, :] = out.astype(BF16)
        o_ref[:, n * HEAD : (n + 1) * HEAD] = out.T.astype(BF16)
        lse_ref[n : n + 1, :] = top_s[n : n + 1, :] * e + jnp.log2(total)


def attend(q, k, v, b=512):
    t, width = q.shape
    b = fit(t, b)
    kv, heads = k.shape[1] // HEAD, width // HEAD
    return call(functools.partial(_attend, kv=kv, g=heads // kv, b=b), (t // b,), [(q, rows(b, width)), (k, kept(k)), (v, kept(v))],
                [rows(b, width), columns(width, b), columns(heads, b)], [shape(t, width), shape(width, t), shape(heads, t, dtype=F32)],
                [pltpu.VMEM((heads, b), F32), pltpu.VMEM((heads, HEAD + 8, b), F32)],
                flops=2 * t * t * width, exps=heads * t * t // 2)


def _feed(o_ref, h_ref, wo_ref, wg_ref, wu_ref, wd_ref, h2_ref, b_ref, gate_ref, up_ref, act_ref, h3_ref, act_s):
    h2 = (h_ref[...].astype(F32) + dot(o_ref[...], wo_ref[...]).astype(BF16).astype(F32)).astype(BF16)
    h2_ref[...] = h2
    b, _ = normed(h2.astype(F32))
    b_ref[...] = b.T
    for at in range(0, wg_ref.shape[1], 512):
        c = slice(at, at + 512)
        gate, up = dot(b, wg_ref[:, c]), dot(b, wu_ref[:, c])
        gate_ref[:, c] = gate
        up_ref[:, c] = up
        act = (gate * sigmoid(gate) * up).astype(BF16)
        act_ref[c, :] = act.T
        if h3_ref is not None:
            act_s[:, c] = act
    if h3_ref is not None:
        h3_ref[...] = (h2.astype(F32) + dot(act_s[...], wd_ref[...]).astype(BF16).astype(F32)).astype(BF16)


def feed(o, h, weights, number, last, bt=256):
    t, d = h.shape
    bt = fit(t, bt)
    wo, wg, wu, wd = weights[3:]
    f = wg.shape[2]
    ins = [(o, rows(bt, o.shape[1])), (h, rows(bt, d)), *(whole(w) for w in ((wo, wg, wu) if last else (wo, wg, wu, wd)))]
    specs = [rows(bt, d), columns(d, bt), rows(bt, f), rows(bt, f), columns(f, bt)] + ([] if last else [rows(bt, d)])
    shapes = [shape(t, d), shape(d, t), shape(t, f, dtype=F32), shape(t, f, dtype=F32), shape(f, t)] + ([] if last else [shape(t, d)])

    def kernel(*refs):
        _feed(*refs[:5], None, *refs[5:], None, None) if last else _feed(*refs)

    return call(kernel, (t // bt,), ins, specs, shapes, [] if last else [pltpu.VMEM((bt, f), BF16)],
                flops=2 * t * d * (o.shape[1] + (2 if last else 3) * f), exps=t * f, number=number)


def _feed_back(dh_ref, h2_ref, gate_ref, up_ref, wo_ref, wg_ref, wu_ref, wd_ref, dgu_ref, dh2_ref, do_ref):
    dh, f = dh_ref[...], wg_ref.shape[1]
    for at in range(0, f, 512):
        c = slice(at, at + 512)
        dact = dot(dh, wd_ref[c, :], 1, 1).astype(BF16).astype(F32)
        gate, up = gate_ref[:, c], up_ref[:, c]
        sig = sigmoid(gate)
        s = gate * sig
        dgu_ref[:, f + at : f + at + 512] = (dact * s).astype(BF16)
        dgu_ref[:, c] = (dact * up * (sig + s * (1 - sig))).astype(BF16)
    db = dot(dgu_ref[:, :f], wg_ref[...], 1, 1) + dot(dgu_ref[:, f:], wu_ref[...], 1, 1)
    by_h = norm_back(h2_ref[...].astype(F32), db.astype(BF16).astype(F32)).astype(BF16)
    dh2 = (dh.astype(F32) + by_h.astype(F32)).astype(BF16)
    dh2_ref[...] = dh2
    do_ref[...] = dot(dh2, wo_ref[...], 1, 1).astype(BF16)


def feed_back(dh, h2, gate, up, weights, number, bt=256):
    t, d = dh.shape
    bt = fit(t, bt)
    f, n = gate.shape[1], weights[3].shape[1]
    return call(_feed_back, (t // bt,),
                [(dh, rows(bt, d)), (h2, rows(bt, d)), (gate, rows(bt, f)), (up, rows(bt, f)), *(whole(w) for w in weights[3:])],
                [rows(bt, 2 * f), rows(bt, d), rows(bt, n)], [shape(t, 2 * f), shape(t, d), shape(t, n)],
                flops=2 * t * d * (3 * f + n), exps=t * f, number=number)


def _attend_back(q_ref, k_ref, v_ref, o_ref, do_ref, lse_ref, cos_ref, sin_ref, dq_ref, dk_ref, dv_ref, dq_s, dk_s, dv_s, *, kv, g, b):
    iq = pl.program_id(0)
    scale = HEAD**-0.5
    e = scale * LOG2E

    @pl.when(iq == 0)
    def _():
        dk_s[...] = jnp.zeros_like(dk_s)
        dv_s[...] = jnp.zeros_like(dv_s)

    dq_s[...] = jnp.zeros_like(dq_s)
    column = lambda n: slice(n * HEAD, (n + 1) * HEAD)
    deltas = [(do_ref[:, column(n)].astype(F32) * o_ref[:, column(n)].astype(F32)).T.sum(0, keepdims=True) for n in range(kv * g)]

    def block(at, size, first, masked):
        width = b - first
        here = pl.ds(at, size)
        if masked:
            ok = lax.broadcasted_iota(jnp.int32, (size, width), 1) >= lax.broadcasted_iota(jnp.int32, (size, width), 0)
        for i in range(kv):
            key, value = k_ref[here, column(i)], v_ref[here, column(i)]
            group = range(i * g, (i + 1) * g)
            qs = [q_ref[first:, column(n)] for n in group]
            dos = [do_ref[first:, column(n)] for n in group]
            scores = [dot(key, x, 1, 1) for x in qs]
            dps = [dot(value, x, 1, 1) for x in dos]
            ps, dss = [], []
            for n, s, dp in zip(group, scores, dps):
                p = jnp.exp2(s * e - lse_ref[n : n + 1, first:])
                if masked:
                    p = jnp.where(ok, p, 0.0)
                ps.append(p.astype(BF16))
                dss.append((p * (dp - deltas[n][:, first:])).astype(BF16))
            dv_s[i, here, :] += dot(jnp.concatenate(ps, 1), jnp.concatenate(dos, 0))
            dk_s[i, here, :] += dot(jnp.concatenate(dss, 1), jnp.concatenate(qs, 0))
            back = key.T
            for n, ds in zip(group, dss):
                dq_s[n, :, first:] += dot(back, ds)

    _spans(iq, b, block)
    mine = pl.ds(pl.multiple_of(iq * b, b), b)
    cos, sin = cos_ref[mine, :], -sin_ref[mine, :]
    for n in range(kv * g):
        dq_ref[:, column(n)] = turn((dq_s[n] * scale).T.astype(BF16), cos, sin)

    @pl.when(iq == pl.num_programs(0) - 1)
    def _():
        for i in range(kv):
            dk_ref[:, column(i)] = turn((dk_s[i] * scale).astype(BF16), cos_ref[...], -sin_ref[...])
            dv_ref[:, column(i)] = dv_s[i].astype(BF16)


def attend_back(q, k, v, o, do, lse, cos, sin, b=512):
    t, width = q.shape
    b = fit(t, b)
    kv, heads = k.shape[1] // HEAD, width // HEAD
    keys = pl.BlockSpec(k.shape, lambda i, _: (0, 0))
    return call(functools.partial(_attend_back, kv=kv, g=heads // kv, b=b), (t // b,),
                [(q, rows(b, width)), (k, kept(k)), (v, kept(v)), (o, rows(b, width)), (do, rows(b, width)),
                 (lse, columns(heads, b)), (cos, kept(cos)), (sin, kept(sin))],
                [rows(b, width), keys, keys], [shape(t, width), shape(*k.shape), shape(*v.shape)],
                [pltpu.VMEM((heads, HEAD, b), F32), pltpu.VMEM((kv, t, HEAD), F32), pltpu.VMEM((kv, t, HEAD), F32)],
                flops=5 * t * t * width, exps=heads * t * t // 2)


def _project_back(dq_ref, dk_ref, dv_ref, h_ref, dh2_ref, wq_ref, wk_ref, wv_ref, dh_ref):
    da = dot(dq_ref[...], wq_ref[...], 1, 1) + dot(dk_ref[...], wk_ref[...], 1, 1) + dot(dv_ref[...], wv_ref[...], 1, 1)
    by_h = norm_back(h_ref[...].astype(F32), da.astype(BF16).astype(F32)).astype(BF16)
    dh_ref[...] = (dh2_ref[...].astype(F32) + by_h.astype(F32)).astype(BF16)


def project_back(dq, dk, dv, h, dh2, weights, number, bt=512):
    t, d = h.shape
    bt = fit(t, bt)
    return call(_project_back, (t // bt,),
                [(dq, rows(bt, dq.shape[1])), (dk, rows(bt, dk.shape[1])), (dv, rows(bt, dv.shape[1])), (h, rows(bt, d)), (dh2, rows(bt, d)),
                 *(whole(w) for w in weights[:3])],
                [rows(bt, d)], [shape(t, d)], flops=2 * t * d * (dq.shape[1] + 2 * dk.shape[1]), number=number)[0]


def _product(a_ref, b_ref, o_ref):
    o_ref[...] = dot(a_ref[...], b_ref[...]).astype(BF16)


def by_columns(a, b, bn=512):
    (m, t), n = a.shape, b.shape[1]
    bn = fit(n, bn)
    return call(_product, (n // bn,), [(a, kept(a)), (b, columns(t, bn))],
                [columns(m, bn)], [shape(m, n)], flops=2 * m * t * n)[0]


def by_rows(a, b, bm=512):
    (m, t), n = a.shape, b.shape[1]
    bm = fit(m, bm)
    return call(_product, (m // bm,), [(a, rows(bm, t)), (b, kept(b))],
                [rows(bm, n)], [shape(m, n)], flops=2 * m * t * n)[0]


def by_attention(a, o, dq, dh2, dk, dv, bn=256):
    m, t = a.shape
    right = (dq, dh2, dk, dv)
    ends, at = [], 0
    for one in right:
        at += one.shape[1] // bn
        ends.append(at)
    starts = [0] + ends[:-1]

    def kernel(a_ref, o_ref, *rest):
        for which in range(4):
            @pl.when((pl.program_id(0) >= starts[which]) & (pl.program_id(0) < ends[which]))
            def _():
                _product(o_ref if which == 1 else a_ref, rest[which], rest[4])

    blocks = [pl.BlockSpec((t, bn), lambda i, _, lo=lo, hi=hi: (0, jnp.clip(i - lo, 0, hi - lo - 1))) for lo, hi in zip(starts, ends)]
    return call(kernel, (at,), [(a, kept(a)), (o, kept(o)), *zip(right, blocks)], [columns(m, bn)], [shape(m, at * bn)], flops=2 * m * t * at * bn)[0]


def _update(me_ref, factor_ref, *refs, count, layers):
    layer = pl.program_id(0)
    gs, refs = refs[:layers], refs[layers:]
    ins, outs = refs[: 3 * count], refs[3 * count :]
    g_s = outs[-1]
    for number in range(layers):
        @pl.when(layer == number)
        def _():
            g_s[...] = gs[number][...].astype(F32) * factor_ref[:1, :1]
    at = 0
    for i in range(count):
        w, m, v = (ref[...] for ref in ins[3 * i : 3 * i + 3])
        here = slice(at, at + m.shape[1])
        at += m.shape[1]
        g, w = g_s[:, here], w.astype(F32)
        m = 0.9 * m + 0.1 * g
        v = 0.95 * v + 0.05 * g * g
        outs[1 + 2 * i][...] = m
        outs[2 + 2 * i][...] = v
        outs[0][:, here] = (w - 0.02 * (m * lax.rsqrt(v + 1e-8) + 0.1 * w)).astype(BF16)


def update(me, factor, gradients, members, column):
    layers, r, _ = members[0][1].shape
    total = sum(m.shape[2] for _, m, _ in members)
    bt = r // 2
    steps = r // bt
    block = lambda n: pl.BlockSpec((None, bt, n), lambda l, i, me: (l, i, 0))
    ins, specs = [], []
    for number, g in enumerate(gradients):
        ins.append(g)
        specs.append(pl.BlockSpec((bt, total), lambda l, i, me, number=number: (jnp.where(l == number, i, jnp.where(l < number, 0, steps - 1)), column // total)))
    for w, m, v in members:
        n = m.shape[2]
        ins += [w, m, v]
        specs += [pl.BlockSpec((None, bt, n), lambda l, i, me: (l, me[0] * steps + i, 0)), block(n), block(n)]
    outs = [shape(layers, r, total)] + [shape(*m.shape, dtype=F32) for _, m, _ in members for _ in range(2)]
    return pl.pallas_call(
        functools.partial(_update, count=len(members), layers=layers),
        grid_spec=pltpu.PrefetchScalarGridSpec(
            num_scalar_prefetch=1, grid=(layers, steps),
            in_specs=[pl.BlockSpec((8, 128), lambda l, i, me: (0, 0)), *specs],
            out_specs=[block(total)] + [block(m.shape[2]) for _, m, _ in members for _ in range(2)],
            scratch_shapes=[pltpu.VMEM((bt, total), F32)]),
        out_shape=outs,
        compiler_params=pltpu.CompilerParams(dimension_semantics=("arbitrary", "arbitrary"), vmem_limit_bytes=VMEM),
        cost_estimate=pl.CostEstimate(flops=0, transcendentals=layers * r * total, bytes_accessed=22 * layers * r * total),
    )(me, factor, *ins)


def _place(own_ref, left_ref, right_ref, top_ref, bottom_ref, *outs):
    me, n, r = lax.axis_index("dp"), lax.axis_size("dp"), own_ref.shape[0]
    at = 0
    for out in outs:
        here = slice(at, at + out.shape[1])
        at += out.shape[1]
        for source, ref, low in ((0, own_ref, 0), (n - 1, left_ref, 0), (1, right_ref, 0), (2, top_ref, 0), (2, bottom_ref, r // 2)):
            first = pl.multiple_of(lax.rem(me + source, n) * r + low, r // 2)
            out[pl.ds(first, ref.shape[0]), :] = ref[:, here]


def place(pieces, widths, n):
    layers, r, total = pieces[0].shape
    block = lambda rows, columns: pl.BlockSpec((None, rows, columns), lambda l, _: (l, 0, 0))
    return call(_place, (layers,), [(p, block(p.shape[1], total)) for p in pieces], [block(n * r, c) for c in widths],
                [shape(layers, n * r, c) for c in widths])


def gather(own, n):
    right, left = [(i, (i + 1) % n) for i in range(n)], [(i, (i - 1) % n) for i in range(n)]
    half = own.shape[1] // 2
    a = lax.ppermute(own, "dp", right)
    b = lax.ppermute(own, "dp", left)
    return own, a, b, lax.ppermute(a[:, :half], "dp", right), lax.ppermute(b[:, half:], "dp", left)


def _clip(x_ref, o_ref, all_s, sent, come, here, *, count, n):
    me = lax.axis_index("dp")
    others = [lax.rem(me + k, n) for k in range(1, n)]
    barrier = pltpu.get_barrier_semaphore()
    for other in others:
        pl.semaphore_signal(barrier, inc=1, device_id={"dp": other}, device_id_type=pl.DeviceIdType.MESH)
    pl.semaphore_wait(barrier, n - 1)
    own = pltpu.make_async_copy(x_ref, all_s.at[me], here)
    own.start()
    copies = [pltpu.make_async_remote_copy(src_ref=x_ref, dst_ref=all_s.at[me], send_sem=sent.at[k], recv_sem=come.at[k],
                                           device_id={"dp": other}, device_id_type=pl.DeviceIdType.MESH) for k, other in enumerate(others)]
    for copy in copies:
        copy.start()
    own.wait()
    for copy in copies:
        copy.wait()
    squares = all_s[0]
    for k in range(1, n):
        squares = squares + all_s[k]
    o_ref[...] = jnp.minimum(1.0, 0.5 * lax.rsqrt(squares / count + 1e-30))


def clip(squares, count):
    n = lax.axis_size("dp")
    spec = pl.BlockSpec(memory_space=pltpu.VMEM)
    return pl.pallas_call(
        functools.partial(_clip, count=count, n=n), in_specs=[spec], out_specs=spec, out_shape=shape(8, 128, dtype=F32),
        scratch_shapes=[pltpu.VMEM((n, 8, 128), F32), pltpu.SemaphoreType.DMA((n - 1,)), pltpu.SemaphoreType.DMA((n - 1,)), pltpu.SemaphoreType.DMA],
        compiler_params=pltpu.CompilerParams(collective_id=0, has_side_effects=True),
    )(squares)


def solution(mesh):
    def scattered(w):
        return lax.psum_scatter(w, "dp", scatter_dimension=0, tiled=True)

    def step(x, dy, *arrays):
        weights, m, v = (arrays[i : i + 7] for i in (0, 7, 14))
        layers = weights[0].shape[0]
        h, saved = x[0], []
        cos, sin = tables(h.shape[0])
        for number in range(layers):
            q, k, value, a = project(h, weights, number, cos, sin)
            o, turned, lse = attend(q, k, value)
            h2, b, gate, up, act, *out = feed(o, h, weights, number, number == layers - 1)
            saved.append((h, q, k, value, a, o, turned, lse, h2, b, gate, up, act))
            h = out[0] if out else None
        dh, downs, gus, qkvos = dy[0], [None] * layers, [None] * layers, [None] * layers
        together = lax.optimization_barrier
        for number in reversed(range(layers)):
            h, q, k, value, a, o, turned, lse, h2, b, gate, up, act = saved[number]
            before = number + 1 if number + 1 < layers else None
            dh, w_down = together((dh, by_rows(act, dh)))
            downs[number] = scattered(w_down)
            dgu, dh2, do = feed_back(dh, h2, gate, up, weights, number)
            if before is None:
                dgu, downs[number] = together((dgu, downs[number]))
            else:
                dgu, qkvos[before] = together((dgu, qkvos[before]))
            do, w_gu = together((do, by_columns(b, dgu)))
            gus[number] = scattered(w_gu)
            dq, dk, dv = attend_back(q, k, value, o, do, lse, cos, sin)
            if before is not None:
                dq, downs[number] = together((dq, downs[number]))
            w_qkvo = by_attention(a, turned, dq, dh2, dk, dv)
            if number:
                dq, w_qkvo = together((dq, w_qkvo))
                dh = project_back(dq, dk, dv, h, dh2, weights, number)
                dh, gus[number] = together((dh, gus[number]))
            qkvos[number] = scattered(w_qkvo)
        n = lax.axis_size("dp")
        parts = downs + gus + qkvos
        squares = jnp.full((8, 128), sum(jnp.sum(g.astype(F32) ** 2) for g in parts))
        factor = clip(squares, n * sum(g.size for g in parts))
        me = lax.axis_index("dp").astype(jnp.int32).reshape(1)
        new = [None] * 21
        f = weights[4].shape[2]
        token = factor
        d = weights[0].shape[2] + weights[3].shape[2]
        groups = ((qkvos, d, (1, 2)), (gus, 0, (4,)), (gus, f, (5,)), (downs, 0, (6,)), (qkvos, 0, (0, 3)))
        for gradients, column, which in groups:
            own, *moments = update(me, token, gradients, [(weights[i], m[i], v[i]) for i in which], column)
            own, token = together((own, token))
            for at, i in enumerate(which):
                new[7 + i], new[14 + i] = moments[2 * at], moments[2 * at + 1]
            pieces = gather(own, n)
            for i, one in zip(which, place(pieces, [weights[i].shape[2] for i in which], n)):
                new[i] = one
        return tuple(new)

    states, all_of, cut = P(("rep", "dp"), None, None), P(None, None, None), P(None, "dp", None)
    return jax.shard_map(
        step,
        mesh=mesh,
        in_specs=(states, states) + (all_of,) * 7 + (cut,) * 14,
        out_specs=(P("rep", None, None),) * 7 + (P("rep", "dp", None),) * 14,
        check_vma=False,
    )
```

```python
import functools

import jax
import jax.numpy as jnp
from jax import lax
from jax.experimental import pallas as pl
from jax.experimental.pallas import tpu as pltpu
from jax.sharding import PartitionSpec as P


HEAD = 128
THETA = 10000
EPS = 1e-6
LOG2E = 1.4426950408889634
LOW = -1e30
VMEM = 60 * 2**20
F32, BF16 = jnp.float32, jnp.bfloat16


def dot(a, b, ca=1, cb=0):
    return lax.dot_general(a, b, (((ca,), (cb,)), ((), ())), preferred_element_type=F32)


def fit(size, want):
    while size % want:
        want //= 2
    return want


def call(kernel, grid, ins, outs, out_shape, scratch=(), flops=0, exps=0, number=0):
    arrays = [a for a, _ in ins]
    moved = sum(a.size * a.dtype.itemsize for a in arrays) + sum(o.size * o.dtype.itemsize for o in out_shape)
    return pl.pallas_call(
        lambda _, *refs: kernel(*refs),
        grid_spec=pltpu.PrefetchScalarGridSpec(num_scalar_prefetch=1, grid=grid, in_specs=[s for _, s in ins], out_specs=outs, scratch_shapes=list(scratch)),
        out_shape=out_shape,
        compiler_params=pltpu.CompilerParams(dimension_semantics=("arbitrary",) * len(grid), vmem_limit_bytes=VMEM),
        cost_estimate=pl.CostEstimate(flops=flops, transcendentals=exps, bytes_accessed=moved),
    )(jnp.full((1,), number, jnp.int32), *arrays)


def rows(bt, width):
    return pl.BlockSpec((bt, width), lambda i, _: (i, 0))


def columns(height, bt):
    return pl.BlockSpec((height, bt), lambda i, _: (0, i))


def whole(w):
    return w, pl.BlockSpec((None, *w.shape[1:]), lambda i, number: (number[0], 0, 0), pipeline_mode=pl.Buffered(1))


def kept(a):
    return pl.BlockSpec(a.shape, lambda i, _: (0, 0), pipeline_mode=pl.Buffered(1))


def shape(*s, dtype=BF16):
    return jax.ShapeDtypeStruct(s, dtype)


def sigmoid(x):
    return 0.5 * jnp.tanh(0.5 * x) + 0.5


def normed(h):
    scale = lax.rsqrt(jnp.mean(h * h, -1, keepdims=True) + EPS)
    return (h * scale).astype(BF16), scale


def norm_back(h, by_b):
    scale = lax.rsqrt(jnp.mean(h * h, -1, keepdims=True) + EPS)
    along = jnp.mean(h * by_b, -1, keepdims=True)
    return (by_b - h * (along * scale * scale)) * scale


def turn(t, cos, sin):
    t = t.astype(F32)
    return (t * cos + pltpu.roll(t, HEAD // 2, 1) * sin).astype(BF16)


def tables(tokens):
    half, step = HEAD // 2, 64
    rate = THETA ** (-jnp.arange(half, dtype=F32) / half)
    rate, sign = jnp.concatenate([rate, rate]), jnp.concatenate([-jnp.ones(half, F32), jnp.ones(half, F32)])
    coarse = (jnp.arange(tokens // step, dtype=F32) * step)[:, None] * rate
    fine = jnp.arange(step, dtype=F32)[:, None] * rate
    cc, sc, cf, sf = lax.optimization_barrier((jnp.cos(coarse), jnp.sin(coarse) * sign, jnp.cos(fine), jnp.sin(fine)))
    cos = cc[:, None] * cf - sc[:, None] * sign * sf
    sin = sc[:, None] * cf + cc[:, None] * sign * sf
    return cos.reshape(tokens, HEAD), sin.reshape(tokens, HEAD)


def _project(h_ref, wq_ref, wk_ref, wv_ref, cos_ref, sin_ref, q_ref, k_ref, v_ref, a_ref):
    a, _ = normed(h_ref[...].astype(F32))
    a_ref[...] = a.T
    cos, sin = cos_ref[...], sin_ref[...]
    for w_ref, o_ref in ((wq_ref, q_ref), (wk_ref, k_ref)):
        t = dot(a, w_ref[...]).astype(BF16)
        for at in range(0, t.shape[1], HEAD):
            o_ref[:, at : at + HEAD] = turn(t[:, at : at + HEAD], cos, sin)
    v_ref[...] = dot(a, wv_ref[...]).astype(BF16)


def project(h, weights, number, cos, sin, bt=512):
    t, d = h.shape
    bt = fit(t, bt)
    wq, wk, wv = weights[:3]
    nq, nk = wq.shape[2], wk.shape[2]
    return call(_project, (t // bt,),
                [(h, rows(bt, d)), whole(wq), whole(wk), whole(wv), (cos, rows(bt, HEAD)), (sin, rows(bt, HEAD))],
                [rows(bt, nq), rows(bt, nk), rows(bt, nk), columns(d, bt)], [shape(t, nq), shape(t, nk), shape(t, nk), shape(d, t)],
                flops=2 * t * d * (nq + 2 * nk), number=number)


def _spans(iq, b, block):
    lax.fori_loop(0, iq, lambda j, _: block(pl.multiple_of(j * b, b), b, 0, False), None)
    block(pl.multiple_of(iq * b, b), b // 2, 0, True)
    block(pl.multiple_of(iq * b + b // 2, b // 2), b // 2, b // 2, True)


def _attend(q_ref, k_ref, v_ref, o_ref, turned_ref, lse_ref, top_s, mix_s, *, kv, g, b):
    e = HEAD**-0.5 * LOG2E
    heads = [(i, i * g + n) for i in range(kv) for n in range(g)]
    top_s[...] = jnp.full(top_s.shape, LOW, F32)
    mix_s[...] = jnp.zeros(mix_s.shape, F32)

    def block(at, size, first, masked):
        width = b - first
        here = pl.ds(at, size)
        scores = [dot(k_ref[here, i * HEAD : (i + 1) * HEAD], q_ref[first:, n * HEAD : (n + 1) * HEAD], 1, 1) for i, n in heads]
        if masked:
            ok = lax.broadcasted_iota(jnp.int32, (size, width), 1) >= lax.broadcasted_iota(jnp.int32, (size, width), 0)
        parts, keeps = [], []
        for (_, n), s in zip(heads, scores):
            if masked:
                s = jnp.where(ok, s, 2 * LOW)
            old = top_s[n : n + 1, first:]
            top = jnp.maximum(old, s.max(axis=0, keepdims=True))
            top_s[n : n + 1, first:] = top
            parts.append(jnp.exp2((s - top) * e).astype(BF16))
            keeps.append(jnp.exp2((old - top) * e))
        ones = jnp.ones((8, size), BF16)
        values = [jnp.concatenate([v_ref[here, i * HEAD : (i + 1) * HEAD].T, ones], axis=0) for i in range(kv)]
        for (i, n), p, keep in zip(heads, parts, keeps):
            mix_s[n, :, first:] = mix_s[n, :, first:] * keep + dot(values[i], p)

    _spans(pl.program_id(0), b, block)
    for i, n in heads:
        total = mix_s[n, HEAD : HEAD + 1, :]
        out = mix_s[n, :HEAD, :] * (1 / total)
        turned_ref[n * HEAD : (n + 1) * HEAD, :] = out.astype(BF16)
        o_ref[:, n * HEAD : (n + 1) * HEAD] = out.T.astype(BF16)
        lse_ref[n : n + 1, :] = top_s[n : n + 1, :] * e + jnp.log2(total)


def attend(q, k, v, b=512):
    t, width = q.shape
    b = fit(t, b)
    kv, heads = k.shape[1] // HEAD, width // HEAD
    return call(functools.partial(_attend, kv=kv, g=heads // kv, b=b), (t // b,), [(q, rows(b, width)), (k, kept(k)), (v, kept(v))],
                [rows(b, width), columns(width, b), columns(heads, b)], [shape(t, width), shape(width, t), shape(heads, t, dtype=F32)],
                [pltpu.VMEM((heads, b), F32), pltpu.VMEM((heads, HEAD + 8, b), F32)],
                flops=2 * t * t * width, exps=heads * t * t // 2)


def _feed(o_ref, h_ref, wo_ref, wg_ref, wu_ref, wd_ref, h2_ref, b_ref, gate_ref, up_ref, act_ref, h3_ref, act_s):
    h2 = (h_ref[...].astype(F32) + dot(o_ref[...], wo_ref[...]).astype(BF16).astype(F32)).astype(BF16)
    h2_ref[...] = h2
    b, _ = normed(h2.astype(F32))
    b_ref[...] = b.T
    for at in range(0, wg_ref.shape[1], 1024):
        c = slice(at, at + 1024)
        gate, up = dot(b, wg_ref[:, c]), dot(b, wu_ref[:, c])
        gate_ref[:, c] = gate
        up_ref[:, c] = up
        act = (gate * sigmoid(gate) * up).astype(BF16)
        act_ref[c, :] = act.T
        if h3_ref is not None:
            act_s[:, c] = act
    if h3_ref is not None:
        h3_ref[...] = (h2.astype(F32) + dot(act_s[...], wd_ref[...]).astype(BF16).astype(F32)).astype(BF16)


def feed(o, h, weights, number, last, bt=512):
    t, d = h.shape
    bt = fit(t, bt)
    wo, wg, wu, wd = weights[3:]
    f = wg.shape[2]
    ins = [(o, rows(bt, o.shape[1])), (h, rows(bt, d)), *(whole(w) for w in ((wo, wg, wu) if last else (wo, wg, wu, wd)))]
    specs = [rows(bt, d), columns(d, bt), rows(bt, f), rows(bt, f), columns(f, bt)] + ([] if last else [rows(bt, d)])
    shapes = [shape(t, d), shape(d, t), shape(t, f, dtype=F32), shape(t, f, dtype=F32), shape(f, t)] + ([] if last else [shape(t, d)])

    def kernel(*refs):
        _feed(*refs[:5], None, *refs[5:], None, None) if last else _feed(*refs)

    return call(kernel, (t // bt,), ins, specs, shapes, [] if last else [pltpu.VMEM((bt, f), BF16)],
                flops=2 * t * d * (o.shape[1] + (2 if last else 3) * f), exps=t * f, number=number)


def _feed_back(dh_ref, h2_ref, gate_ref, up_ref, wo_ref, wg_ref, wu_ref, wd_ref, dgu_ref, dh2_ref, do_ref):
    dh, f = dh_ref[...], wg_ref.shape[1]
    for at in range(0, f, 1024):
        c = slice(at, at + 1024)
        dact = dot(dh, wd_ref[c, :], 1, 1).astype(BF16).astype(F32)
        gate, up = gate_ref[:, c], up_ref[:, c]
        sig = sigmoid(gate)
        s = gate * sig
        dgu_ref[:, f + at : f + at + 1024] = (dact * s).astype(BF16)
        dgu_ref[:, c] = (dact * up * (sig + s * (1 - sig))).astype(BF16)
    db = dot(dgu_ref[:, :f], wg_ref[...], 1, 1) + dot(dgu_ref[:, f:], wu_ref[...], 1, 1)
    by_h = norm_back(h2_ref[...].astype(F32), db.astype(BF16).astype(F32)).astype(BF16)
    dh2 = (dh.astype(F32) + by_h.astype(F32)).astype(BF16)
    dh2_ref[...] = dh2
    do_ref[...] = dot(dh2, wo_ref[...], 1, 1).astype(BF16)


def feed_back(dh, h2, gate, up, weights, number, bt=512):
    t, d = dh.shape
    bt = fit(t, bt)
    f, n = gate.shape[1], weights[3].shape[1]
    return call(_feed_back, (t // bt,),
                [(dh, rows(bt, d)), (h2, rows(bt, d)), (gate, rows(bt, f)), (up, rows(bt, f)), *(whole(w) for w in weights[3:])],
                [rows(bt, 2 * f), rows(bt, d), rows(bt, n)], [shape(t, 2 * f), shape(t, d), shape(t, n)],
                flops=2 * t * d * (3 * f + n), exps=t * f, number=number)


def _attend_back(q_ref, k_ref, v_ref, o_ref, do_ref, lse_ref, cos_ref, sin_ref, dq_ref, dk_ref, dv_ref, dq_s, dk_s, dv_s, *, kv, g, b):
    iq = pl.program_id(0)
    scale = HEAD**-0.5
    e = scale * LOG2E

    @pl.when(iq == 0)
    def _():
        dk_s[...] = jnp.zeros_like(dk_s)
        dv_s[...] = jnp.zeros_like(dv_s)

    dq_s[...] = jnp.zeros_like(dq_s)
    column = lambda n: slice(n * HEAD, (n + 1) * HEAD)
    deltas = [(do_ref[:, column(n)].astype(F32) * o_ref[:, column(n)].astype(F32)).T.sum(0, keepdims=True) for n in range(kv * g)]

    def block(at, size, first, masked):
        width = b - first
        here = pl.ds(at, size)
        if masked:
            ok = lax.broadcasted_iota(jnp.int32, (size, width), 1) >= lax.broadcasted_iota(jnp.int32, (size, width), 0)
        for i in range(kv):
            key, value = k_ref[here, column(i)], v_ref[here, column(i)]
            group = range(i * g, (i + 1) * g)
            qs = [q_ref[first:, column(n)] for n in group]
            dos = [do_ref[first:, column(n)] for n in group]
            scores = [dot(key, x, 1, 1) for x in qs]
            dps = [dot(value, x, 1, 1) for x in dos]
            ps, dss = [], []
            for n, s, dp in zip(group, scores, dps):
                p = jnp.exp2(s * e - lse_ref[n : n + 1, first:])
                if masked:
                    p = jnp.where(ok, p, 0.0)
                ps.append(p.astype(BF16))
                dss.append((p * (dp - deltas[n][:, first:])).astype(BF16))
            dv_s[i, here, :] += dot(jnp.concatenate(ps, 1), jnp.concatenate(dos, 0))
            dk_s[i, here, :] += dot(jnp.concatenate(dss, 1), jnp.concatenate(qs, 0))
            back = key.T
            for n, ds in zip(group, dss):
                dq_s[n, :, first:] += dot(back, ds)

    _spans(iq, b, block)
    mine = pl.ds(pl.multiple_of(iq * b, b), b)
    cos, sin = cos_ref[mine, :], -sin_ref[mine, :]
    for n in range(kv * g):
        dq_ref[:, column(n)] = turn((dq_s[n] * scale).T.astype(BF16), cos, sin)

    @pl.when(iq == pl.num_programs(0) - 1)
    def _():
        for i in range(kv):
            dk_ref[:, column(i)] = turn((dk_s[i] * scale).astype(BF16), cos_ref[...], -sin_ref[...])
            dv_ref[:, column(i)] = dv_s[i].astype(BF16)


def attend_back(q, k, v, o, do, lse, cos, sin, b=512):
    t, width = q.shape
    b = fit(t, b)
    kv, heads = k.shape[1] // HEAD, width // HEAD
    keys = pl.BlockSpec(k.shape, lambda i, _: (0, 0))
    return call(functools.partial(_attend_back, kv=kv, g=heads // kv, b=b), (t // b,),
                [(q, rows(b, width)), (k, kept(k)), (v, kept(v)), (o, rows(b, width)), (do, rows(b, width)),
                 (lse, columns(heads, b)), (cos, kept(cos)), (sin, kept(sin))],
                [rows(b, width), keys, keys], [shape(t, width), shape(*k.shape), shape(*v.shape)],
                [pltpu.VMEM((heads, HEAD, b), F32), pltpu.VMEM((kv, t, HEAD), F32), pltpu.VMEM((kv, t, HEAD), F32)],
                flops=5 * t * t * width, exps=heads * t * t // 2)


def _project_back(dq_ref, dk_ref, dv_ref, h_ref, dh2_ref, wq_ref, wk_ref, wv_ref, dh_ref):
    da = dot(dq_ref[...], wq_ref[...], 1, 1) + dot(dk_ref[...], wk_ref[...], 1, 1) + dot(dv_ref[...], wv_ref[...], 1, 1)
    by_h = norm_back(h_ref[...].astype(F32), da.astype(BF16).astype(F32)).astype(BF16)
    dh_ref[...] = (dh2_ref[...].astype(F32) + by_h.astype(F32)).astype(BF16)


def project_back(dq, dk, dv, h, dh2, weights, number, bt=512):
    t, d = h.shape
    bt = fit(t, bt)
    return call(_project_back, (t // bt,),
                [(dq, rows(bt, dq.shape[1])), (dk, rows(bt, dk.shape[1])), (dv, rows(bt, dv.shape[1])), (h, rows(bt, d)), (dh2, rows(bt, d)),
                 *(whole(w) for w in weights[:3])],
                [rows(bt, d)], [shape(t, d)], flops=2 * t * d * (dq.shape[1] + 2 * dk.shape[1]), number=number)[0]


def _product(a_ref, b_ref, o_ref):
    o_ref[...] = dot(a_ref[...], b_ref[...]).astype(BF16)


def by_columns(a, b, bn=512):
    (m, t), n = a.shape, b.shape[1]
    bn = fit(n, bn)
    return call(_product, (n // bn,), [(a, kept(a)), (b, columns(t, bn))],
                [columns(m, bn)], [shape(m, n)], flops=2 * m * t * n)[0]


def by_rows(a, b, bm=512):
    (m, t), n = a.shape, b.shape[1]
    bm = fit(m, bm)
    return call(_product, (m // bm,), [(a, rows(bm, t)), (b, kept(b))],
                [rows(bm, n)], [shape(m, n)], flops=2 * m * t * n)[0]


def by_attention(a, o, dq, dh2, dk, dv, bn=256):
    m, t = a.shape
    right = (dq, dh2, dk, dv)
    ends, at = [], 0
    for one in right:
        at += one.shape[1] // bn
        ends.append(at)
    starts = [0] + ends[:-1]

    def kernel(a_ref, o_ref, *rest):
        for which in range(4):
            @pl.when((pl.program_id(0) >= starts[which]) & (pl.program_id(0) < ends[which]))
            def _():
                _product(o_ref if which == 1 else a_ref, rest[which], rest[4])

    blocks = [pl.BlockSpec((t, bn), lambda i, _, lo=lo, hi=hi: (0, jnp.clip(i - lo, 0, hi - lo - 1))) for lo, hi in zip(starts, ends)]
    return call(kernel, (at,), [(a, kept(a)), (o, kept(o)), *zip(right, blocks)], [columns(m, bn)], [shape(m, at * bn)], flops=2 * m * t * at * bn)[0]


def _update(me_ref, factor_ref, *refs, count, layers):
    layer = pl.program_id(0)
    gs, refs = refs[:layers], refs[layers:]
    ins, outs = refs[: 3 * count], refs[3 * count :]
    g_s = outs[-1]
    for number in range(layers):
        @pl.when(layer == number)
        def _():
            g_s[...] = gs[number][...].astype(F32) * factor_ref[:1, :1]
    at = 0
    for i in range(count):
        w, m, v = (ref[...] for ref in ins[3 * i : 3 * i + 3])
        here = slice(at, at + m.shape[1])
        at += m.shape[1]
        g, w = g_s[:, here], w.astype(F32)
        m = 0.9 * m + 0.1 * g
        v = 0.95 * v + 0.05 * g * g
        outs[1 + 2 * i][...] = m
        outs[2 + 2 * i][...] = v
        outs[0][:, here] = (w - 0.02 * (m * lax.rsqrt(v + 1e-8) + 0.1 * w)).astype(BF16)


def update(me, factor, gradients, members, column):
    layers, r, _ = members[0][1].shape
    total = sum(m.shape[2] for _, m, _ in members)
    bt = r // 2
    steps = r // bt
    block = lambda n: pl.BlockSpec((None, bt, n), lambda l, i, me: (l, i, 0))
    ins, specs = [], []
    for number, g in enumerate(gradients):
        ins.append(g)
        specs.append(pl.BlockSpec((bt, total), lambda l, i, me, number=number: (jnp.where(l == number, i, jnp.where(l < number, 0, steps - 1)), column // total)))
    for w, m, v in members:
        n = m.shape[2]
        ins += [w, m, v]
        specs += [pl.BlockSpec((None, bt, n), lambda l, i, me: (l, me[0] * steps + i, 0)), block(n), block(n)]
    outs = [shape(layers, r, total)] + [shape(*m.shape, dtype=F32) for _, m, _ in members for _ in range(2)]
    return pl.pallas_call(
        functools.partial(_update, count=len(members), layers=layers),
        grid_spec=pltpu.PrefetchScalarGridSpec(
            num_scalar_prefetch=1, grid=(layers, steps),
            in_specs=[pl.BlockSpec((8, 128), lambda l, i, me: (0, 0)), *specs],
            out_specs=[block(total)] + [block(m.shape[2]) for _, m, _ in members for _ in range(2)],
            scratch_shapes=[pltpu.VMEM((bt, total), F32)]),
        out_shape=outs,
        compiler_params=pltpu.CompilerParams(dimension_semantics=("arbitrary", "arbitrary"), vmem_limit_bytes=VMEM),
        cost_estimate=pl.CostEstimate(flops=0, transcendentals=layers * r * total, bytes_accessed=22 * layers * r * total),
    )(me, factor, *ins)


def _place(own_ref, left_ref, right_ref, top_ref, bottom_ref, *outs):
    me, n, r = lax.axis_index("dp"), lax.axis_size("dp"), own_ref.shape[0]
    at = 0
    for out in outs:
        here = slice(at, at + out.shape[1])
        at += out.shape[1]
        for source, ref, low in ((0, own_ref, 0), (n - 1, left_ref, 0), (1, right_ref, 0), (2, top_ref, 0), (2, bottom_ref, r // 2)):
            first = pl.multiple_of(lax.rem(me + source, n) * r + low, r // 2)
            out[pl.ds(first, ref.shape[0]), :] = ref[:, here]


def place(pieces, widths, n):
    layers, r, total = pieces[0].shape
    block = lambda rows, columns: pl.BlockSpec((None, rows, columns), lambda l, _: (l, 0, 0))
    return call(_place, (layers,), [(p, block(p.shape[1], total)) for p in pieces], [block(n * r, c) for c in widths],
                [shape(layers, n * r, c) for c in widths])


def gather(own, n):
    right, left = [(i, (i + 1) % n) for i in range(n)], [(i, (i - 1) % n) for i in range(n)]
    half = own.shape[1] // 2
    a = lax.ppermute(own, "dp", right)
    b = lax.ppermute(own, "dp", left)
    c = lax.ppermute(a[:, :half], "dp", right)
    d = lax.ppermute(b[:, half:], "dp", left)
    return own, a, b, c, d


def _clip(x_ref, o_ref, all_s, sent, come, here, *, count, n):
    me = lax.axis_index("dp")
    others = [lax.rem(me + k, n) for k in range(1, n)]
    barrier = pltpu.get_barrier_semaphore()
    for other in others:
        pl.semaphore_signal(barrier, inc=1, device_id={"dp": other}, device_id_type=pl.DeviceIdType.MESH)
    pl.semaphore_wait(barrier, n - 1)
    own = pltpu.make_async_copy(x_ref, all_s.at[me], here)
    own.start()
    copies = [pltpu.make_async_remote_copy(src_ref=x_ref, dst_ref=all_s.at[me], send_sem=sent.at[k], recv_sem=come.at[k],
                                           device_id={"dp": other}, device_id_type=pl.DeviceIdType.MESH) for k, other in enumerate(others)]
    for copy in copies:
        copy.start()
    own.wait()
    for copy in copies:
        copy.wait()
    squares = all_s[0]
    for k in range(1, n):
        squares = squares + all_s[k]
    o_ref[...] = jnp.minimum(1.0, 0.5 * lax.rsqrt(squares / count + 1e-30))


def clip(squares, count):
    n = lax.axis_size("dp")
    spec = pl.BlockSpec(memory_space=pltpu.VMEM)
    return pl.pallas_call(
        functools.partial(_clip, count=count, n=n), in_specs=[spec], out_specs=spec, out_shape=shape(8, 128, dtype=F32),
        scratch_shapes=[pltpu.VMEM((n, 8, 128), F32), pltpu.SemaphoreType.DMA((n - 1,)), pltpu.SemaphoreType.DMA((n - 1,)), pltpu.SemaphoreType.DMA],
        compiler_params=pltpu.CompilerParams(collective_id=0, has_side_effects=True),
    )(squares)


def solution(mesh):
    def scattered(w):
        return lax.psum_scatter(w, "dp", scatter_dimension=0, tiled=True)

    def step(x, dy, *arrays):
        weights, m, v = (arrays[i : i + 7] for i in (0, 7, 14))
        layers = weights[0].shape[0]
        h, saved = x[0], []
        cos, sin = tables(h.shape[0])
        for number in range(layers):
            q, k, value, a = project(h, weights, number, cos, sin)
            o, turned, lse = attend(q, k, value)
            h2, b, gate, up, act, *out = feed(o, h, weights, number, number == layers - 1)
            saved.append((h, q, k, value, a, o, turned, lse, h2, b, gate, up, act))
            h = out[0] if out else None
        dh, downs, gus, qkvos = dy[0], [None] * layers, [None] * layers, [None] * layers
        together = lax.optimization_barrier
        for number in reversed(range(layers)):
            h, q, k, value, a, o, turned, lse, h2, b, gate, up, act = saved[number]
            before = number + 1 if number + 1 < layers else None
            dh, w_down = together((dh, by_rows(act, dh)))
            downs[number] = scattered(w_down)
            dgu, dh2, do = feed_back(dh, h2, gate, up, weights, number)
            if before is None:
                dgu, downs[number] = together((dgu, downs[number]))
            else:
                dgu, qkvos[before] = together((dgu, qkvos[before]))
            do, w_gu = together((do, by_columns(b, dgu)))
            gus[number] = scattered(w_gu)
            dq, dk, dv = attend_back(q, k, value, o, do, lse, cos, sin)
            if before is not None:
                dq, downs[number] = together((dq, downs[number]))
            w_qkvo = by_attention(a, turned, dq, dh2, dk, dv)
            if number:
                dq, w_qkvo = together((dq, w_qkvo))
                dh = project_back(dq, dk, dv, h, dh2, weights, number)
                dh, gus[number] = together((dh, gus[number]))
            qkvos[number] = scattered(w_qkvo)
        n = lax.axis_size("dp")
        parts = downs + gus + qkvos
        squares = jnp.full((8, 128), sum(jnp.sum(g.astype(F32) ** 2) for g in parts))
        factor = clip(squares, n * sum(g.size for g in parts))
        me = lax.axis_index("dp").astype(jnp.int32).reshape(1)
        new = [None] * 21
        f = weights[4].shape[2]
        token = factor
        d = weights[0].shape[2] + weights[3].shape[2]
        groups = ((qkvos, d, (1, 2)), (gus, 0, (4,)), (gus, f, (5,)), (downs, 0, (6,)), (qkvos, 0, (0, 3)))
        for gradients, column, which in groups:
            own, *moments = update(me, token, gradients, [(weights[i], m[i], v[i]) for i in which], column)
            own, token = together((own, token))
            for at, i in enumerate(which):
                new[7 + i], new[14 + i] = moments[2 * at], moments[2 * at + 1]
            pieces = gather(own, n)
            placed = place(pieces, [weights[i].shape[2] for i in which], n)
            for i, one in zip(which, placed):
                new[i] = one
        return tuple(new)

    states, all_of, cut = P(("rep", "dp"), None, None), P(None, None, None), P(None, "dp", None)
    return jax.shard_map(
        step,
        mesh=mesh,
        in_specs=(states, states) + (all_of,) * 7 + (cut,) * 14,
        out_specs=(P("rep", None, None),) * 7 + (P("rep", "dp", None),) * 14,
        check_vma=False,
    )
```
